32 devices in a mesh: groups: 2 (over x), rows: 4 (over y, core), cols: 4 (over z).
Axes of the slice: x: 2, y: 2, z: 4, core: 2. Of those that a mesh axis runs over, the one named last changes fastest.
Arguments:
- pair_state: float32 [768, 384, 128], P(('groups', 'rows'), 'cols'), parts along dimension 0, may hold values from -6 to 6
- token_mask: int32 [768], P('groups'), parts along dimension 0, may hold values 0 or 1
- norm_gain: float32 [2, 128], replicated, may hold values from 0.25 to 1.75
- norm_bias: float32 [2, 128], replicated, may hold values from -3 to 3
- proj_weight: float32 [2, 128, 512], replicated, may hold values from -0.5 to 0.5
- gate_weight: float32 [2, 128, 128], replicated, may hold values from -0.5 to 0.5
- out_gain: float32 [2, 128], replicated, may hold values from 0.25 to 1.75
- out_bias: float32 [2, 128], replicated, may hold values from -3 to 3
- out_weight: float32 [2, 128, 128], replicated, may hold values from -0.5 to 0.5
Outputs:
- pair_out: float32 [768, 384, 128], P(('groups', 'rows'), 'cols'), parts along dimension 0
The draws below stay inside these ranges and needn't reach their ends.
There are 2 independent parts, one for each index of `groups`. The reference program is written for one: setup_inputs(seed, part) draws one part's arguments, and reference() takes and returns one part's arrays. A program takes and returns all parts, laid end to end along the dimension named above; an argument that names none is the same for every part. Nothing has to cross between parts.
All inputs are finite; a program needn't handle non-finite values.
Results may differ from the reference program's by a relative error of at most 0.0001.
Values sent between devices are 32-bit elements; how exact they have to be, the bound alone decides.
A program may use at most 128 MiB of HBM per device.

```python
import jax
import jax.numpy as jnp
from jax import lax

C = 128
H = 128
N = 384


def plant(array, rng, least, high):
    shape = array.shape
    place = [jax.random.randint(jax.random.fold_in(rng, axis), (), 0, shape[axis]) for axis in range(len(shape))]
    array = array.at[tuple(place)].set(least)
    longest = shape.index(max(shape))
    place[longest] = (place[longest] + 1) % shape[longest]
    return array.at[tuple(place)].set(high)


def block_scale(stream_key, extent, pieces, smallest, top_value):
    def one(axis_at, shards_of):
        draws = jax.random.uniform(jax.random.fold_in(jax.random.fold_in(stream_key, 6), axis_at), (shards_of,), jnp.float32, smallest / len(pieces), top_value / len(pieces))
        return jnp.repeat(jnp.exp(draws), extent[axis_at] // shards_of).reshape((-1,) + (1,) * (len(extent) - axis_at - 1))

    level = one(*pieces[0])
    for cut in pieces[1:]:
        level = level * one(*cut)
    return level


def scatter_about(rng, shape, scale, limit, cuts=(), dtype=jnp.bfloat16):
    level = block_scale(rng, shape, cuts, -0.22, 0.18) if cuts else 1.0
    values = jax.random.normal(rng, shape, jnp.float32) * scale * level
    return jnp.minimum(jnp.maximum(values, -limit), limit).astype(dtype)


def setup_inputs(seed: int = 0, part: int = 0) -> dict:
    streams_of = jax.random.split(jax.random.key(seed), 10)
    part_keys = jax.random.split(jax.random.fold_in(streams_of[9], part), 10)
    return {
        "pair_state": scatter_about(part_keys[0], (N, N, C), 1.0, 6.0, ((0, 4), (1, 4)), jnp.float32),
        "token_mask": plant((jax.random.randint(part_keys[1], (N,), 0, 4) < 3).astype(jnp.int32), jax.random.fold_in(part_keys[1], 1), 0, 1),
        "norm_gain": jnp.clip(1.0 + 0.15 * jax.random.normal(streams_of[2], (2, C), jnp.float32), 0.25, 1.75),
        "norm_bias": scatter_about(streams_of[3], (2, C), 0.5, 3.0, (), jnp.float32),
        "proj_weight": scatter_about(streams_of[4], (2, C, 4 * H), C ** -0.5, 0.5, (), jnp.float32),
        "gate_weight": scatter_about(streams_of[5], (2, C, C), C ** -0.5, 0.5, (), jnp.float32),
        "out_gain": jnp.clip(1.0 + 0.15 * jax.random.normal(streams_of[6], (2, H), jnp.float32), 0.25, 1.75),
        "out_bias": scatter_about(streams_of[7], (2, H), 0.5, 3.0, (), jnp.float32),
        "out_weight": scatter_about(streams_of[8], (2, H, C), H ** -0.5, 0.5, (), jnp.float32),
    }


eps = 1e-05

def normalize(values, gain, shift):
    center = values - lax.optimization_barrier(jnp.mean(values, axis=-1, keepdims=True))
    spread = lax.optimization_barrier(jnp.mean(center * center, axis=-1, keepdims=True))
    return center * lax.rsqrt(spread + eps) * gain + shift

def update_once(state, pair_mask, segment, norm_gain, norm_bias, proj_weight, gate_weight, out_gain, out_bias, out_weight):
    width = proj_weight.shape[2] // 4
    normed = normalize(state, norm_gain[segment], norm_bias[segment])
    hidden = jnp.einsum('ijc,cf->ijf', normed, proj_weight[segment], precision=lax.Precision.HIGHEST)
    left_side = pair_mask[:, :, None] * jax.nn.sigmoid(hidden[:, :, :width]) * hidden[:, :, width:2 * width]
    right_side = pair_mask[:, :, None] * jax.nn.sigmoid(hidden[:, :, 2 * width:3 * width]) * hidden[:, :, 3 * width:]
    gating = jax.nn.sigmoid(jnp.einsum('ijc,cd->ijd', normed, gate_weight[segment], precision=lax.Precision.HIGHEST))
    if segment == 0:
        mixed = jnp.einsum('ikh,jkh->ijh', left_side, right_side, precision=lax.Precision.HIGHEST)
    else:
        mixed = jnp.einsum('kih,kjh->ijh', left_side, right_side, precision=lax.Precision.HIGHEST)
    result = jnp.einsum('ijh,hc->ijc', normalize(mixed, out_gain[segment], out_bias[segment]), out_weight[segment], precision=lax.Precision.HIGHEST)
    return state + gating * result

def reference(pair_state, token_mask, norm_gain, norm_bias, proj_weight, gate_weight, out_gain, out_bias, out_weight):
    maskf = token_mask.astype(jnp.float32)
    pair_mask = maskf[:, None] * maskf[None, :]
    state = pair_state
    for segment in range(2):
        state = update_once(state, pair_mask, segment, norm_gain, norm_bias, proj_weight, gate_weight, out_gain, out_bias, out_weight)
    return state
```

```python
import functools

import jax
import jax.numpy as jnp
from jax import lax
from jax.experimental import pallas as pl
from jax.experimental.pallas import tpu as pltpu
from jax.sharding import PartitionSpec as P

eps = 1e-05
precise = lax.Precision.HIGH
MESH = pl.DeviceIdType.MESH
LANES = 128
VMEM_LIMIT = 67_000_000


def normalize(values, gain, shift):
    center = values - jnp.mean(values, axis=-1, keepdims=True)
    spread = jnp.mean(center * center, axis=-1, keepdims=True)
    return center * lax.rsqrt(spread + eps) * gain + shift


def project(state, pair_mask, segment, norm_gain, norm_bias, proj_weight, gate_weight):
    width = proj_weight.shape[2] // 4
    normed = normalize(state, norm_gain[segment], norm_bias[segment])
    hidden = jnp.einsum(
        "ijc,cf->ijf", normed, proj_weight[segment], precision=precise
    )
    left_side = (
        pair_mask[:, :, None]
        * jax.nn.sigmoid(hidden[:, :, :width])
        * hidden[:, :, width : 2 * width]
    )
    right_side = (
        pair_mask[:, :, None]
        * jax.nn.sigmoid(hidden[:, :, 2 * width : 3 * width])
        * hidden[:, :, 3 * width :]
    )
    gating = jax.nn.sigmoid(
        jnp.einsum("ijc,cd->ijd", normed, gate_weight[segment], precision=precise)
    )
    return (left_side, right_side, gating)


def finish(state, mixed, gating, segment, out_gain, out_bias, out_weight):
    result = jnp.einsum(
        "ijh,hc->ijc",
        normalize(mixed, out_gain[segment], out_bias[segment]),
        out_weight[segment],
        precision=precise,
    )
    return state + gating * result


def plain_body(
    pair_state,
    token_mask,
    norm_gain,
    norm_bias,
    proj_weight,
    gate_weight,
    out_gain,
    out_bias,
    out_weight,
):
    row_count = pair_state.shape[0]
    col_count = pair_state.shape[1]
    row_start = lax.axis_index("rows") * row_count
    col_start = lax.axis_index("cols") * col_count
    maskf = token_mask.astype(jnp.float32)
    row_mask = lax.dynamic_slice_in_dim(maskf, row_start, row_count)
    col_mask = lax.dynamic_slice_in_dim(maskf, col_start, col_count)
    pair_mask = row_mask[:, None] * col_mask[None, :]
    left_side, right_side, gating = project(
        pair_state, pair_mask, 0, norm_gain, norm_bias, proj_weight, gate_weight
    )
    partial_out = jnp.einsum(
        "ikh,jkh->ijh",
        left_side,
        lax.all_gather(right_side, "rows", axis=0, tiled=True),
        precision=precise,
    )
    mixed = lax.psum_scatter(partial_out, "cols", scatter_dimension=1, tiled=True)
    updated = finish(pair_state, mixed, gating, 0, out_gain, out_bias, out_weight)
    left_next, right_next, gate_next = project(
        updated, pair_mask, 1, norm_gain, norm_bias, proj_weight, gate_weight
    )
    partial_in = jnp.einsum(
        "kih,kjh->ijh",
        lax.all_gather(left_next, "cols", axis=1, tiled=True),
        right_next,
        precision=precise,
    )
    mixed_next = lax.psum_scatter(partial_in, "rows", scatter_dimension=0, tiled=True)
    return finish(updated, mixed_next, gate_next, 1, out_gain, out_bias, out_weight)


def halves(x):
    high = x.astype(jnp.bfloat16)
    return high, (x - high.astype(jnp.float32)).astype(jnp.bfloat16)


def streamed(x):
    high, low = halves(x)
    return jnp.concatenate([high, low, high], axis=1)


def held(x):
    high, low = halves(x)
    return jnp.concatenate([high, high, low], axis=1)


def stacked(weight):
    rounded = lax.reduce_precision(weight, 8, 7)
    high, low = rounded.astype(jnp.bfloat16), (weight - rounded).astype(jnp.bfloat16)
    return jnp.concatenate([high, high, low], axis=0)


def times(x, weight3):
    return jnp.dot(streamed(x), weight3, preferred_element_type=jnp.float32)


def against(a3, b3):
    return lax.dot_general(
        a3, b3, (((1,), (1,)), ((), ())), preferred_element_type=jnp.float32
    )


def gated_three(normed, mask, weight3):
    hidden = times(normed, weight3)
    part = lambda f: hidden[:, f * LANES : (f + 1) * LANES]
    return (
        mask * jax.nn.sigmoid(part(0)) * part(1),
        mask * jax.nn.sigmoid(part(2)) * part(3),
        jax.nn.sigmoid(part(4)),
    )


def padded(x):
    rows = x.shape[0]
    if rows == LANES:
        return x
    return jnp.concatenate([x, jnp.zeros((LANES - rows, x.shape[1]), x.dtype)], axis=0)


def first_kernel(group, state, rmask, cmask, vec, weight3, left_t, right_t, gate):
    m, extent, _ = state.shape
    count = group * extent

    @pl.loop(0, m // group)
    def _(g):
        x = state[pl.ds(g * group, group)].reshape(count, LANES)
        normed = normalize(x, vec[0:1, :], vec[1:2, :])
        mask = (rmask[pl.ds(g * group, group)] * cmask[...][None]).reshape(count, LANES)
        left, right, gating = gated_three(normed, mask, weight3[...])
        gate[pl.ds(g * group, group)] = gating.reshape(group, extent, LANES)
        for b in range(group):
            rows = slice(b * extent, (b + 1) * extent)
            left_t[0, pl.ds(g * group + b, LANES, m), :] = padded(left[rows]).T
            right_t[0, pl.ds(g * group + b, LANES, m), :] = padded(right[rows]).T


def first_call(n, state, rmask, cmask, vec, weight3):
    extent = state.shape[0]
    m = extent // n
    turned = jax.ShapeDtypeStruct((n, LANES * m, LANES), jnp.float32)
    whole = lambda a: pl.BlockSpec(a.shape, lambda p: (0,) * a.ndim)
    return pl.pallas_call(
        functools.partial(first_kernel, 4),
        grid=(n,),
        in_specs=[
            pl.BlockSpec((m, extent, LANES), lambda p: (p, 0, 0)),
            pl.BlockSpec((m, 1, LANES), lambda p: (p, 0, 0)),
            whole(cmask), whole(vec), whole(weight3),
        ],
        out_specs=[
            pl.BlockSpec((1, LANES * m, LANES), lambda p: (p, 0, 0)),
            pl.BlockSpec((1, LANES * m, LANES), lambda p: (p, 0, 0)),
            pl.BlockSpec((m, extent, LANES), lambda p: (p, 0, 0)),
        ],
        out_shape=[turned, turned, jax.ShapeDtypeStruct(state.shape, jnp.float32)],
        compiler_params=pltpu.CompilerParams(vmem_limit_bytes=VMEM_LIMIT),
    )(state, rmask, cmask, vec, weight3)


def middle_kernel(
    rows, cols, n, parts,
    left_t, right_t, state, gate0, rmask, cmask, vec, out3, proj3,
    near, line, lefts, rights, state1, gate1,
    high, low, block, turned, chunk, from_left, from_right, tile, done,
    gather_send, gather_recv, load_sem, tile_sem,
    sum_send_r, sum_send_l, sum_recv_r, sum_recv_l,
    line_recv_r, line_recv_l, done_sem, forward_sem, spread_sem, left_recv, right_recv,
):
    m = tile.shape[2]
    extent = n * m
    ticks = n * parts
    last = cols - 1
    r, c = lax.axis_index("rows"), lax.axis_index("cols")
    back = last - c
    partner = r + 1 - 2 * lax.rem(r, 2)
    across = lax.rem(r + 2, rows)
    beyond = lax.rem(partner + 2, rows)

    barrier = pltpu.get_barrier_semaphore()
    for off in range(1, rows):
        pl.semaphore_signal(barrier, inc=1, device_id={"rows": lax.rem(r + off, rows)}, device_id_type=MESH)

    @pl.when(c > 0)
    def _():
        pl.semaphore_signal(barrier, inc=1, device_id={"cols": c - 1}, device_id_type=MESH)

    @pl.when(c < last)
    def _():
        pl.semaphore_signal(barrier, inc=1, device_id={"cols": c + 1}, device_id_type=MESH)

    pl.semaphore_wait(barrier, rows - 1 + jnp.minimum(c, 1) + jnp.minimum(back, 1))

    def remote(src, dst, send, recv, **where):
        return pltpu.make_async_remote_copy(
            src_ref=src, dst_ref=dst, send_sem=send, recv_sem=recv,
            device_id=where, device_id_type=MESH,
        )

    def to_partner(p):
        return remote(right_t.at[p], near.at[r, p], gather_send.at[0, p], gather_recv.at[0, p], rows=partner)

    def to_across(p):
        return remote(right_t.at[p], near.at[r, p], gather_send.at[1, p], gather_recv.at[1, p], rows=across)

    def relay(p):
        return remote(near.at[across, p], near.at[across, p], gather_send.at[2, p], gather_recv.at[2, p], rows=partner)

    def loads(p):
        return [
            pltpu.make_async_copy(right_t.at[p], block.at[r], load_sem.at[0]),
            pltpu.make_async_copy(near.at[partner, p], block.at[partner], load_sem.at[1]),
            pltpu.make_async_copy(near.at[across, p], block.at[across], load_sem.at[2]),
            pltpu.make_async_copy(near.at[beyond, p], block.at[beyond], load_sem.at[3]),
        ]

    for p in range(n):
        to_across(p).start()
        to_partner(p).start()

    fill = [
        pltpu.make_async_copy(left_t.at[p], turned.at[pl.ds(p * LANES * m, LANES * m)], load_sem.at[p])
        for p in range(n)
    ]
    for copy in fill:
        copy.start()
    for copy in fill:
        copy.wait()

    @pl.loop(0, LANES)
    def _(h):
        rows_of = [
            turned[pl.ds(pl.multiple_of(p * LANES * m + h * m, 8), m), :] for p in range(n)
        ]
        top, rest = halves(jnp.concatenate(rows_of, axis=0))
        high[h] = top
        low[h] = rest

    to_across(0).wait_recv()
    relay(0).start()
    to_partner(0).wait_recv()
    relay(0).wait_recv()
    for copy in loads(0):
        copy.start()

    def multiply():
        @pl.loop(0, LANES // 4)
        def _(g):
            for b in range(4):
                h = g * 4 + b
                at = pl.multiple_of(h * m, 8)
                right = padded(jnp.concatenate([block[o, pl.ds(at, m), :] for o in range(rows)], axis=0))
                a3 = jnp.concatenate([high[h], low[h], high[h]], axis=1)
                turned[pl.ds(h, extent, LANES), :] = against(a3, held(right))

    def turn(q, slot):
        @pl.loop(0, m)
        def _(i):
            at = pl.multiple_of((q * m + i) * LANES, LANES)
            straight = turned[pl.ds(at, LANES), :].T
            for d in range(cols):
                chunk[slot, d, i] = straight[d * m : (d + 1) * m]

    def sum_right(u, s):
        slot = lax.rem(u, 4)
        return remote(chunk.at[slot, c + last - s], from_left.at[u, s], sum_send_r.at[slot, s], sum_recv_r.at[u, s], cols=c + 1)

    def sum_left(u, s):
        slot = lax.rem(u, 4)
        return remote(chunk.at[slot, c - last + s], from_right.at[u, s], sum_send_l.at[slot, s], sum_recv_l.at[u, s], cols=c - 1)

    def arrived_right(u, s):
        return remote(chunk.at[0, 0], from_left.at[u, s], sum_send_r.at[0, s], sum_recv_r.at[u, s], cols=c - 1)

    def arrived_left(u, s):
        return remote(chunk.at[0, 0], from_right.at[u, s], sum_send_l.at[0, s], sum_recv_l.at[u, s], cols=c + 1)

    def add_to(slot, d, source, u, s):
        @pl.loop(0, m)
        def _(i):
            chunk[slot, d, i] = chunk[slot, d, i] + source[u, s, i]

    def pass_sums(u, s):
        slot = lax.rem(u, 4)

        @pl.when(c <= s)
        def _():
            if s:
                @pl.when(c > 0)
                def _():
                    arrived_right(u, s - 1).wait_recv()
                    add_to(slot, c + last - s, from_left, u, s - 1)
            sum_right(u, s).start()

        @pl.when(back <= s)
        def _():
            if s:
                @pl.when(back > 0)
                def _():
                    arrived_left(u, s - 1).wait_recv()
                    add_to(slot, c - last + s, from_right, u, s - 1)
            sum_left(u, s).start()

    def clear_sums(u):
        for s in range(last):
            @pl.when(c <= s)
            def _():
                sum_right(u, s).wait_send()

            @pl.when(back <= s)
            def _():
                sum_left(u, s).wait_send()

    def own_sum(u):
        slot = lax.rem(u, 4)

        @pl.when(c > 0)
        def _():
            arrived_right(u, last - 1).wait_recv()
            add_to(slot, c, from_left, u, last - 1)

        @pl.when(c < last)
        def _():
            arrived_left(u, last - 1).wait_recv()
            add_to(slot, c, from_right, u, last - 1)

    def spot(u):
        p, q = u // parts, lax.rem(u, parts)
        return pl.ds(pl.multiple_of(q * m, 8), m), pl.ds(pl.multiple_of(p * m, 8), m)

    def tiles(u):
        i, j = spot(u)
        return [
            pltpu.make_async_copy(state.at[i, j], tile.at[0], tile_sem.at[0]),
            pltpu.make_async_copy(gate0.at[i, j], tile.at[1], tile_sem.at[1]),
        ]

    def line_right(u, s):
        src = done.at[lax.rem(u, 2), 0] if s == 0 else line.at[c - s, u]
        send = done_sem.at[lax.rem(u, 2), 0] if s == 0 else forward_sem.at[0]
        return remote(src, line.at[c - s, u], send, line_recv_r.at[u, s], cols=c + 1)

    def line_left(u, s):
        src = done.at[lax.rem(u, 2), 0] if s == 0 else line.at[c + s, u]
        send = done_sem.at[lax.rem(u, 2), 1] if s == 0 else forward_sem.at[1]
        return remote(src, line.at[c + s, u], send, line_recv_l.at[u, s], cols=c - 1)

    def own_spread(u):
        return remote(done.at[lax.rem(u, 2), 0], lefts.at[r, u], done_sem.at[lax.rem(u, 2), 2], left_recv.at[r], rows=c)

    def own_keep(u):
        return pltpu.make_async_copy(done.at[lax.rem(u, 2), 0], line.at[c, u], done_sem.at[lax.rem(u, 2), 3])

    def right_to(u, off):
        return remote(
            done.at[lax.rem(u, 2), 1], rights.at[r, u], done_sem.at[lax.rem(u, 2), 3 + off],
            right_recv.at[r], rows=lax.rem(r + off, rows),
        )

    def kept(u):
        i, j = spot(u)
        slot = lax.rem(u, 2)
        return [
            pltpu.make_async_copy(done.at[slot, 1], rights.at[r, u], done_sem.at[slot, 7]),
            pltpu.make_async_copy(done.at[slot, 2], state1.at[i, j], done_sem.at[slot, 8]),
            pltpu.make_async_copy(done.at[slot, 3], gate1.at[i, j], done_sem.at[slot, 9]),
        ]

    def each_send(u, act):
        @pl.when(c < last)
        def _():
            act(line_right(u, 0), True)

        @pl.when(c > 0)
        def _():
            act(line_left(u, 0), True)

        @pl.when(c != r)
        def _():
            act(own_spread(u), True)

        @pl.when(c == r)
        def _():
            act(own_keep(u), False)

        for off in range(1, rows):
            act(right_to(u, off), True)
        for copy in kept(u):
            act(copy, False)

    start = lambda copy, away: copy.start()
    sent = lambda copy, away: copy.wait_send() if away else copy.wait()
    few = 8

    def update(u):
        slot, out = lax.rem(u, 4), lax.rem(u, 2)
        p, q = u // parts, lax.rem(u, parts)
        count = few * m

        @pl.loop(0, m // few)
        def _(g):
            at = pl.ds(g * few, few)
            mixed = chunk[slot, c, at].reshape(count, LANES)
            result = times(normalize(mixed, vec[0:1, :], vec[1:2, :]), out3[...])
            new = tile[0, at].reshape(count, LANES) + tile[1, at].reshape(count, LANES) * result
            normed = normalize(new, vec[2:3, :], vec[3:4, :])
            row_part = rmask[pl.ds(q * m + g * few, few)]
            col_part = cmask[pl.ds(pl.multiple_of(p * m, 8), m), :]
            mask = (row_part * col_part[None]).reshape(count, LANES)
            left, right, gating = gated_three(normed, mask, proj3[...])
            for k, value in enumerate((left, right, new, gating)):
                done[out, k, at] = value.reshape(few, m, LANES)

    def pass_line(u, s):
        @pl.when(c >= s)
        def _():
            line_right_in(u, s - 1).wait_recv()
            if s < last:
                @pl.when(c < last)
                def _():
                    line_right(u, s).start()
            spread(u, c - s)

        @pl.when(back >= s)
        def _():
            line_left_in(u, s - 1).wait_recv()
            if s < last:
                @pl.when(back < last)
                def _():
                    line_left(u, s).start()
            spread(u, c + s)

    def line_right_in(u, s):
        return remote(done.at[0, 0], line.at[c - 1 - s, u], forward_sem.at[0], line_recv_r.at[u, s], cols=c - 1)

    def line_left_in(u, s):
        return remote(done.at[0, 0], line.at[c + 1 + s, u], forward_sem.at[1], line_recv_l.at[u, s], cols=c + 1)

    def spread(u, origin):
        @pl.when(origin != r)
        def _():
            remote(line.at[origin, u], lefts.at[r, u], spread_sem, left_recv.at[r], rows=origin).start()

    def within(u):
        return jnp.logical_and(u >= 0, u < ticks)

    @pl.loop(0, ticks + 2 * last + 1)
    def _(t):
        p, q = t // parts, lax.rem(t, parts)

        @pl.when(within(t - last))
        def _():
            for copy in tiles(t - last):
                copy.start()

        @pl.when(within(t - 4))
        def _():
            clear_sums(t - 4)

        @pl.when(t < ticks)
        def _():
            @pl.when(q == 0)
            def _():
                for copy in loads(p):
                    copy.wait()
                multiply()

            turn(q, lax.rem(t, 4))
            pass_sums(t, 0)

            @pl.when(jnp.logical_and(q == 1, p + 1 < n))
            def _():
                to_across(p + 1).wait_recv()
                relay(p + 1).start()

            @pl.when(jnp.logical_and(q == parts - 1, p + 1 < n))
            def _():
                to_partner(p + 1).wait_recv()
                relay(p + 1).wait_recv()
                for copy in loads(p + 1):
                    copy.start()

        for s in range(1, last):
            @pl.when(within(t - s))
            def _():
                pass_sums(t - s, s)

        for s in range(1, last + 1):
            @pl.when(within(t - last - s))
            def _():
                pass_line(t - last - s, s)

        u = t - last

        @pl.when(within(u - 2))
        def _():
            each_send(u - 2, sent)

        @pl.when(within(u))
        def _():
            own_sum(u)
            for copy in tiles(u):
                copy.wait()
            update(u)
            each_send(u, start)

    for p in range(n):
        to_across(p).wait_send()
        to_partner(p).wait_send()
        relay(p).wait_send()

    def drain(sem, count):
        pltpu.make_async_copy(line.at[pl.ds(0, count)], line.at[pl.ds(0, count)], sem).wait()

    for count in range(1, last):
        @pl.when(c == count)
        def _():
            drain(forward_sem.at[0], count)

        @pl.when(back == count)
        def _():
            drain(forward_sem.at[1], count)

    @pl.when(c == r)
    def _():
        drain(spread_sem, last)

    @pl.when(c != r)
    def _():
        drain(spread_sem, last - 1)

    for other in range(rows):
        @pl.when(r != other)
        def _():
            pltpu.make_async_copy(lefts.at[other], lefts.at[other], left_recv.at[other]).wait()
            pltpu.make_async_copy(rights.at[other], rights.at[other], right_recv.at[other]).wait()


def middle_call(rows, cols, n, parts, left_t, right_t, state, gate0, rmask, cmask, vec, out3, proj3):
    extent = state.shape[0]
    m = extent // n
    ticks = n * parts
    last = cols - 1
    f32 = jnp.float32
    bit = (m, m, LANES)
    anywhere = pl.BlockSpec(memory_space=pl.ANY)
    inside = pl.BlockSpec(memory_space=pltpu.VMEM)
    dma = pltpu.SemaphoreType.DMA
    return pl.pallas_call(
        functools.partial(middle_kernel, rows, cols, n, parts),
        in_specs=[anywhere] * 4 + [inside] * 5,
        out_specs=[anywhere] * 6,
        out_shape=[
            jax.ShapeDtypeStruct((rows, n, LANES * m, LANES), f32),
            jax.ShapeDtypeStruct((cols, ticks) + bit, f32),
            jax.ShapeDtypeStruct((rows, ticks) + bit, f32),
            jax.ShapeDtypeStruct((rows, ticks) + bit, f32),
            jax.ShapeDtypeStruct(state.shape, f32),
            jax.ShapeDtypeStruct(state.shape, f32),
        ],
        scratch_shapes=[
            pltpu.VMEM((LANES, extent, LANES), jnp.bfloat16),
            pltpu.VMEM((LANES, extent, LANES), jnp.bfloat16),
            pltpu.VMEM((rows, LANES * m, LANES), f32),
            pltpu.VMEM((extent * LANES, LANES), f32),
            pltpu.VMEM((4, cols) + bit, f32),
            pltpu.VMEM((ticks, last) + bit, f32),
            pltpu.VMEM((ticks, last) + bit, f32),
            pltpu.VMEM((2,) + bit, f32),
            pltpu.VMEM((2, 4) + bit, f32),
            dma((3, n)), dma((3, n)), dma((4,)), dma((2,)),
            dma((4, last)), dma((4, last)), dma((ticks, last)), dma((ticks, last)),
            dma((ticks, last)), dma((ticks, last)), dma((2, 10)), dma((2,)), dma,
            dma((rows,)), dma((rows,)),
        ],
        compiler_params=pltpu.CompilerParams(
            collective_id=0, has_side_effects=True, vmem_limit_bytes=VMEM_LIMIT
        ),
    )(left_t, right_t, state, gate0, rmask, cmask, vec, out3, proj3)


def last_kernel(rows, n, parts, lefts, line, rights, state1, gate1, vec, out3, out, *scratch):
    left_k, right_k, turned = scratch[0:rows - 1], scratch[rows - 1 : 2 * rows - 2], scratch[2 * rows - 2]
    flat, load_sem = scratch[2 * rows - 1 : 2 * rows + 1]
    extent = state1.shape[0]
    m = extent // n
    r = lax.axis_index("rows")
    depth = rows * extent
    wide = depth // LANES

    def each_load(which, p, act):
        for o in range(rows):
            into = flat.at[which, pl.ds(o * extent * m, extent * m)]

            def copy(source):
                view = source.at[o, p]
                act(pltpu.make_async_copy(view, into, load_sem.at[which, o]))

            if which:
                copy(rights)
            else:
                @pl.when(r == o)
                def _():
                    copy(line)

                @pl.when(r != o)
                def _():
                    copy(lefts)

    start = lambda copy: copy.start()
    wait = lambda copy: copy.wait()
    for which in range(2):
        each_load(which, 0, start)

    @pl.loop(0, n)
    def _(p):
        for which, target in enumerate((left_k, right_k)):
            each_load(which, p, wait)

            @pl.loop(0, m)
            def _(i):
                for w in range(wide):
                    got = flat[which, pl.ds(w * LANES * m + i, LANES, m), :].T
                    target[w][pl.ds(p * m + i, LANES, extent), :] = got

            @pl.when(p + 1 < n)
            def _():
                each_load(which, p + 1, start)

    size = extent * extent
    ends = [
        pltpu.make_async_copy(source, flat.at[k, pl.ds(0, size)], load_sem.at[k, 0])
        for k, source in enumerate((state1.reshape(size, LANES), gate1.reshape(size, LANES)))
    ]
    for copy in ends:
        copy.start()

    @pl.loop(0, LANES // 2)
    def _(g):
        for b in range(2):
            h = g * 2 + b
            at = pl.ds(pl.multiple_of(h * extent, 8), extent)
            a = [halves(left_k[w][at, :]) for w in range(wide)]
            k = [halves(padded(right_k[w][at, :])) for w in range(wide)]
            a3 = jnp.concatenate([x[0] for x in a] + [x[1] for x in a] + [x[0] for x in a], axis=1)
            k3 = jnp.concatenate([x[0] for x in k] + [x[0] for x in k] + [x[1] for x in k], axis=1)
            turned[pl.ds(h, extent, LANES), :] = against(a3, k3)

    for copy in ends:
        copy.wait()

    few = 4

    @pl.loop(0, extent // few)
    def _(g):
        straight = [
            turned[pl.ds(pl.multiple_of((g * few + b) * LANES, LANES), LANES), :].T[:extent]
            for b in range(few)
        ]
        mixed = jnp.concatenate(straight, axis=0)
        result = times(normalize(mixed, vec[0:1, :], vec[1:2, :]), out3[...])
        at = pl.ds(pl.multiple_of(g * few * extent, 8), few * extent)
        out[at, :] = flat[0, at, :] + flat[1, at, :] * result


def last_call(rows, n, parts, lefts, line, rights, state1, gate1, vec, out3):
    extent = state1.shape[0]
    m = extent // n
    f32 = jnp.float32
    anywhere = pl.BlockSpec(memory_space=pl.ANY)
    inside = pl.BlockSpec(memory_space=pltpu.VMEM)
    wide = rows * extent // LANES
    pieces = lambda a: a.reshape(rows, n, parts * m * m, LANES)
    out = pl.pallas_call(
        functools.partial(last_kernel, rows, n, parts),
        in_specs=[anywhere] * 5 + [inside] * 2,
        out_specs=inside,
        out_shape=jax.ShapeDtypeStruct((extent * extent, LANES), f32),
        scratch_shapes=[pltpu.VMEM((LANES * extent, LANES), f32)] * (2 * wide + 1)
        + [pltpu.VMEM((2, rows * extent * m, LANES), f32), pltpu.SemaphoreType.DMA((2, rows))],
        compiler_params=pltpu.CompilerParams(vmem_limit_bytes=VMEM_LIMIT),
    )(pieces(lefts), pieces(line), pieces(rights), state1, gate1, vec, out3)
    return out.reshape(extent, extent, LANES)


def body(rows, cols, pieces, pair_state, token_mask, norm_gain, norm_bias, proj_weight,
         gate_weight, out_gain, out_bias, out_weight):
    extent = pair_state.shape[0]
    row_at, col_at = lax.axis_index("rows"), lax.axis_index("cols")
    maskf = token_mask.astype(jnp.float32)
    spread = lambda at: jnp.broadcast_to(
        lax.dynamic_slice_in_dim(maskf, at * extent, extent)[:, None], (extent, LANES)
    )
    rmask, cmask = spread(row_at)[:, None, :], spread(col_at)
    full = jnp.concatenate([proj_weight, gate_weight], axis=2)
    left_t, right_t, gate0 = first_call(
        pieces, pair_state, rmask, cmask, jnp.stack([norm_gain[0], norm_bias[0]]), stacked(full[0])
    )
    _, line, lefts, rights, state1, gate1 = middle_call(
        rows, cols, pieces, pieces, left_t, right_t, pair_state, gate0, rmask, cmask,
        jnp.stack([out_gain[0], out_bias[0], norm_gain[1], norm_bias[1]]),
        stacked(out_weight[0]), stacked(full[1]),
    )
    return last_call(
        rows, pieces, pieces, lefts, line, rights, state1, gate1,
        jnp.stack([out_gain[1], out_bias[1]]), stacked(out_weight[1]),
    )


def solution(mesh):
    placed = (P(("groups", "rows"), "cols", None), P("groups"), P(), P(), P(), P(), P(), P(), P())
    rows, cols = mesh.shape["rows"], mesh.shape["cols"]

    def run(pair_state, *rest):
        proj_weight = rest[3]
        channels, hidden = pair_state.shape[2], proj_weight.shape[2] // 4
        extent = pair_state.shape[0]
        fits = channels == hidden == LANES and extent == pair_state.shape[1] and extent <= LANES
        if rows == cols == 4 and fits and extent % (8 * rows) == 0:
            return body(rows, cols, rows, pair_state, *rest)
        return plain_body(pair_state, *rest)

    return jax.shard_map(
        run,
        mesh=mesh,
        in_specs=placed,
        out_specs=P(("groups", "rows"), "cols", None),
        check_vma=False,
    )
```

```python
import functools

import jax
import jax.numpy as jnp
from jax import lax
from jax.experimental import pallas as pl
from jax.experimental.pallas import tpu as pltpu
from jax.sharding import PartitionSpec as P

eps = 1e-05
precise = lax.Precision.HIGH
MESH = pl.DeviceIdType.MESH
LANES = 128
VMEM_LIMIT = 67_000_000


def normalize(values, gain, shift):
    center = values - jnp.mean(values, axis=-1, keepdims=True)
    spread = jnp.mean(center * center, axis=-1, keepdims=True)
    return center * lax.rsqrt(spread + eps) * gain + shift


def project(state, pair_mask, segment, norm_gain, norm_bias, proj_weight, gate_weight):
    width = proj_weight.shape[2] // 4
    normed = normalize(state, norm_gain[segment], norm_bias[segment])
    hidden = jnp.einsum(
        "ijc,cf->ijf", normed, proj_weight[segment], precision=precise
    )
    left_side = (
        pair_mask[:, :, None]
        * jax.nn.sigmoid(hidden[:, :, :width])
        * hidden[:, :, width : 2 * width]
    )
    right_side = (
        pair_mask[:, :, None]
        * jax.nn.sigmoid(hidden[:, :, 2 * width : 3 * width])
        * hidden[:, :, 3 * width :]
    )
    gating = jax.nn.sigmoid(
        jnp.einsum("ijc,cd->ijd", normed, gate_weight[segment], precision=precise)
    )
    return (left_side, right_side, gating)


def finish(state, mixed, gating, segment, out_gain, out_bias, out_weight):
    result = jnp.einsum(
        "ijh,hc->ijc",
        normalize(mixed, out_gain[segment], out_bias[segment]),
        out_weight[segment],
        precision=precise,
    )
    return state + gating * result


def plain_body(
    pair_state,
    token_mask,
    norm_gain,
    norm_bias,
    proj_weight,
    gate_weight,
    out_gain,
    out_bias,
    out_weight,
):
    row_count = pair_state.shape[0]
    col_count = pair_state.shape[1]
    row_start = lax.axis_index("rows") * row_count
    col_start = lax.axis_index("cols") * col_count
    maskf = token_mask.astype(jnp.float32)
    row_mask = lax.dynamic_slice_in_dim(maskf, row_start, row_count)
    col_mask = lax.dynamic_slice_in_dim(maskf, col_start, col_count)
    pair_mask = row_mask[:, None] * col_mask[None, :]
    left_side, right_side, gating = project(
        pair_state, pair_mask, 0, norm_gain, norm_bias, proj_weight, gate_weight
    )
    partial_out = jnp.einsum(
        "ikh,jkh->ijh",
        left_side,
        lax.all_gather(right_side, "rows", axis=0, tiled=True),
        precision=precise,
    )
    mixed = lax.psum_scatter(partial_out, "cols", scatter_dimension=1, tiled=True)
    updated = finish(pair_state, mixed, gating, 0, out_gain, out_bias, out_weight)
    left_next, right_next, gate_next = project(
        updated, pair_mask, 1, norm_gain, norm_bias, proj_weight, gate_weight
    )
    partial_in = jnp.einsum(
        "kih,kjh->ijh",
        lax.all_gather(left_next, "cols", axis=1, tiled=True),
        right_next,
        precision=precise,
    )
    mixed_next = lax.psum_scatter(partial_in, "rows", scatter_dimension=0, tiled=True)
    return finish(updated, mixed_next, gate_next, 1, out_gain, out_bias, out_weight)


def halves(x):
    high = x.astype(jnp.bfloat16)
    return high, (x - high.astype(jnp.float32)).astype(jnp.bfloat16)


def streamed(x):
    high, low = halves(x)
    return jnp.concatenate([high, low, high], axis=1)


def held(x):
    high, low = halves(x)
    return jnp.concatenate([high, high, low], axis=1)


def stack_into(target, first, weight):
    high, low = halves(weight)
    for k, part in enumerate((high, high, low)):
        target[k * LANES : (k + 1) * LANES, first : first + weight.shape[1]] = part


def times(x, weight3):
    return jnp.dot(streamed(x), weight3, preferred_element_type=jnp.float32)


def against(a3, b3):
    return lax.dot_general(
        a3, b3, (((1,), (1,)), ((), ())), preferred_element_type=jnp.float32
    )


def gated_three(normed, mask, weight3):
    hidden = times(normed, weight3)
    part = lambda f: hidden[:, f * LANES : (f + 1) * LANES]
    return (
        mask * jax.nn.sigmoid(part(0)) * part(1),
        mask * jax.nn.sigmoid(part(2)) * part(3),
        jax.nn.sigmoid(part(4)),
    )


def padded(x):
    rows = x.shape[0]
    if rows == LANES:
        return x
    return jnp.concatenate([x, jnp.zeros((LANES - rows, x.shape[1]), x.dtype)], axis=0)


def middle_kernel(
    rows, cols, n, parts,
    state, tokens, norm_gain, norm_bias, proj, gate_weight, out_gain, out_bias, out_weight,
    near, line, lefts, rights, right_k, state1, gate1, gate0,
    mine, first, opened, first3, high, low, block, turned, stage, chunk, from_left, from_right, tile, done, ready, out3, proj3,
    first_sem, opened_sem, early_send, early_recv, gather_send, gather_recv, load_sem, tile_sem,
    sum_send_r, sum_send_l, sum_recv_r, sum_recv_l,
    line_recv_r, line_recv_l, done_sem, forward_sem, spread_sem, left_recv,
    right_near, right_across, right_beyond, right_relay, stage_sem,
):
    mi, m = tile.shape[1:3]
    extent = n * m
    ticks = n * parts
    last = cols - 1
    r, c = lax.axis_index("rows"), lax.axis_index("cols")
    back = last - c
    depth, ring = done.shape[0], from_left.shape[0]
    partner = r + 1 - 2 * lax.rem(r, 2)
    across = lax.rem(r + 2, rows)
    beyond = lax.rem(partner + 2, rows)

    def opening(p):
        return pltpu.make_async_copy(state.at[pl.ds(p * m, m)], first.at[p % 2], first_sem.at[p % 2])

    opening(0).start()
    stack_into(first3, 0, proj[0])
    stack_into(first3, 4 * LANES, gate_weight[0])
    stack_into(out3, 0, out_weight[0])
    stack_into(proj3, 0, proj[1])
    stack_into(proj3, 4 * LANES, gate_weight[1])

    barrier = pltpu.get_barrier_semaphore()
    for off in range(1, rows):
        pl.semaphore_signal(barrier, inc=1, device_id={"rows": lax.rem(r + off, rows)}, device_id_type=MESH)

    @pl.when(c > 0)
    def _():
        pl.semaphore_signal(barrier, inc=1, device_id={"cols": c - 1}, device_id_type=MESH)

    @pl.when(c < last)
    def _():
        pl.semaphore_signal(barrier, inc=1, device_id={"cols": c + 1}, device_id_type=MESH)

    pl.semaphore_wait(barrier, rows - 1 + jnp.minimum(c, 1) + jnp.minimum(back, 1))

    def remote(src, dst, send, recv, **where):
        return pltpu.make_async_remote_copy(
            src_ref=src, dst_ref=dst, send_sem=send, recv_sem=recv,
            device_id=where, device_id_type=MESH,
        )

    def to_partner(p):
        return remote(mine.at[p], near.at[0, p], gather_send.at[0, p], gather_recv.at[0, p], rows=partner)

    def to_across(p):
        return remote(mine.at[p], near.at[1, p], gather_send.at[1, p], gather_recv.at[1, p], rows=across)

    def relay(p):
        return remote(near.at[1, p], near.at[2, p], gather_send.at[2, p], gather_recv.at[2, p], rows=partner)

    def slab(o):
        return block.at[pl.ds(pl.multiple_of(o * LANES * m, 8), LANES * m)]

    def loads(p):
        return [
            pltpu.make_async_copy(mine.at[p], slab(r), load_sem.at[0]),
            pltpu.make_async_copy(near.at[0, p], slab(partner), load_sem.at[1]),
            pltpu.make_async_copy(near.at[1, p], slab(across), load_sem.at[2]),
            pltpu.make_async_copy(near.at[2, p], slab(beyond), load_sem.at[3]),
        ]

    cuts = 4
    cut = LANES // cuts

    def part(k):
        return pl.ds(k * cut * m, cut * m)

    def early(k):
        return (
            remote(mine.at[0, part(k)], near.at[0, 0, part(k)], early_send.at[0, k], early_recv.at[0, k], rows=partner),
            remote(mine.at[0, part(k)], near.at[1, 0, part(k)], early_send.at[1, k], early_recv.at[1, k], rows=across),
            remote(near.at[1, 0, part(k)], near.at[2, 0, part(k)], early_send.at[2, k], early_recv.at[2, k], rows=partner),
        )

    def early_loads(k):
        return [
            pltpu.make_async_copy(
                source.at[0, part(k)],
                block.at[pl.ds(pl.multiple_of(o * LANES * m + k * cut * m, 8), cut * m)],
                load_sem.at[b],
            )
            for b, (source, o) in enumerate(
                ((mine, r), (near.at[0], partner), (near.at[1], across), (near.at[2], beyond))
            )
        ]

    def closing(p):
        return pltpu.make_async_copy(opened.at[p % 2], gate0.at[pl.ds(p * m, m)], opened_sem.at[p % 2])

    group = 4
    taken = group * extent
    for p in range(n):
        opening(p).wait()
        if p + 1 < n:
            opening(p + 1).start()
        if p >= 2:
            closing(p - 2).wait()

        @pl.loop(0, m // group)
        def _(g):
            rows_at = pl.ds(g * group, group)
            normed = normalize(first[p % 2, rows_at].reshape(taken, LANES), norm_gain[0:1, :], norm_bias[0:1, :])
            row_first = r * extent + p * m + g * group
            col_part = tokens[pl.ds(pl.multiple_of(c * extent, 8), extent), :]
            mask = jnp.concatenate(
                [tokens[pl.ds(row_first + b, 1), :] * col_part for b in range(group)], axis=0
            )
            left, right, gating = gated_three(normed, mask, first3[...])
            opened[p % 2, rows_at] = gating.reshape(group, extent, LANES)
            for b in range(group):
                span = slice(b * extent, (b + 1) * extent)
                mine[p, pl.ds(g * group + b, LANES, m), :] = padded(right[span]).T
                turned[1, pl.ds(p * LANES * m + g * group + b, LANES, m), :] = padded(left[span]).T

        closing(p).start()
        if p:
            to_across(p).start()
            to_partner(p).start()
        else:
            for k in range(cuts):
                for copy in early(k)[1::-1]:
                    copy.start()
    for p in range(max(n - 2, 0), n):
        closing(p).wait()

    @pl.loop(0, LANES)
    def _(h):
        rows_of = [
            turned[1, pl.ds(pl.multiple_of(p * LANES * m + h * m, 8), m), :] for p in range(n)
        ]
        top, rest = halves(jnp.concatenate(rows_of, axis=0))
        high[h] = top
        low[h] = rest

    def multiply(p, start_at, count):
        half = lax.rem(p, 2)

        @pl.loop(start_at // 4, (start_at + count) // 4)
        def _(g):
            for b in range(4):
                h = g * 4 + b
                right = padded(jnp.concatenate(
                    [block[pl.ds(pl.multiple_of(o * LANES * m + h * m, 8), m), :] for o in range(rows)], axis=0
                ))
                a3 = jnp.concatenate([high[h], low[h], high[h]], axis=1)
                turned[half, pl.ds(h, extent, LANES), :] = against(a3, held(right))

    def turn(p, q, slot):
        @pl.loop(0, mi)
        def _(i):
            at = pl.multiple_of((q * mi + i) * LANES, LANES)
            straight = turned[lax.rem(p, 2), pl.ds(at, LANES), :].T
            for d in range(cols):
                chunk[slot, d, i] = straight[d * m : (d + 1) * m]

    def sum_right(u, s):
        slot = lax.rem(u, 4)
        return remote(chunk.at[slot, c + last - s], from_left.at[lax.rem(u, ring), s], sum_send_r.at[slot, s], sum_recv_r.at[lax.rem(u, ring), s], cols=c + 1)

    def sum_left(u, s):
        slot = lax.rem(u, 4)
        return remote(chunk.at[slot, c - last + s], from_right.at[lax.rem(u, ring), s], sum_send_l.at[slot, s], sum_recv_l.at[lax.rem(u, ring), s], cols=c - 1)

    def arrived_right(u, s):
        return remote(chunk.at[0, 0], from_left.at[lax.rem(u, ring), s], sum_send_r.at[0, s], sum_recv_r.at[lax.rem(u, ring), s], cols=c - 1)

    def arrived_left(u, s):
        return remote(chunk.at[0, 0], from_right.at[lax.rem(u, ring), s], sum_send_l.at[0, s], sum_recv_l.at[lax.rem(u, ring), s], cols=c + 1)

    def add_to(slot, d, source, u, s):
        @pl.loop(0, mi)
        def _(i):
            chunk[slot, d, i] = chunk[slot, d, i] + source[lax.rem(u, ring), s, i]

    def pass_sums(u, s):
        slot = lax.rem(u, 4)

        @pl.when(c <= s)
        def _():
            if s:
                @pl.when(c > 0)
                def _():
                    arrived_right(u, s - 1).wait_recv()
                    add_to(slot, c + last - s, from_left, u, s - 1)
            sum_right(u, s).start()

        @pl.when(back <= s)
        def _():
            if s:
                @pl.when(back > 0)
                def _():
                    arrived_left(u, s - 1).wait_recv()
                    add_to(slot, c - last + s, from_right, u, s - 1)
            sum_left(u, s).start()

    def clear_sums(u):
        for s in range(last):
            @pl.when(c <= s)
            def _():
                sum_right(u, s).wait_send()

            @pl.when(back <= s)
            def _():
                sum_left(u, s).wait_send()

    def own_sum(u):
        slot = lax.rem(u, 4)

        @pl.when(c > 0)
        def _():
            arrived_right(u, last - 1).wait_recv()
            add_to(slot, c, from_left, u, last - 1)

        @pl.when(c < last)
        def _():
            arrived_left(u, last - 1).wait_recv()
            add_to(slot, c, from_right, u, last - 1)

    def spot(u):
        p, q = u // parts, lax.rem(u, parts)
        return pl.ds(q * mi, mi), pl.ds(pl.multiple_of(p * m, 8), m)

    def tiles(u):
        i, j = spot(u)
        return [
            pltpu.make_async_copy(state.at[i, j], tile.at[0], tile_sem.at[0]),
            pltpu.make_async_copy(gate0.at[i, j], tile.at[1], tile_sem.at[1]),
        ]

    def at(u):
        return pl.ds(pl.multiple_of(u * mi * m, 8), mi * m)

    def line_right(u, s):
        src = done.at[lax.rem(u, depth), 0] if s == 0 else line.at[c - s, at(u)]
        send = done_sem.at[lax.rem(u, depth), 0] if s == 0 else forward_sem.at[0]
        return remote(src, line.at[c - s, at(u)], send, line_recv_r.at[u, s], cols=c + 1)

    def line_left(u, s):
        src = done.at[lax.rem(u, depth), 0] if s == 0 else line.at[c + s, at(u)]
        send = done_sem.at[lax.rem(u, depth), 1] if s == 0 else forward_sem.at[1]
        return remote(src, line.at[c + s, at(u)], send, line_recv_l.at[u, s], cols=c - 1)

    def own_spread(u):
        return remote(done.at[lax.rem(u, depth), 0], lefts.at[r, at(u)], done_sem.at[lax.rem(u, depth), 2], left_recv.at[r, u // parts], rows=c)

    def own_keep(u):
        return pltpu.make_async_copy(done.at[lax.rem(u, depth), 0], line.at[c, at(u)], done_sem.at[lax.rem(u, depth), 3])

    def right_to_partner(u):
        return remote(done.at[lax.rem(u, depth), 1], rights.at[r, at(u)], done_sem.at[lax.rem(u, depth), 4], right_near.at[u // parts], rows=partner)

    def right_to_across(u):
        return remote(done.at[lax.rem(u, depth), 1], rights.at[r, at(u)], done_sem.at[lax.rem(u, depth), 5], right_across.at[u], rows=across)

    def right_on(u):
        return remote(rights.at[across, at(u)], rights.at[across, at(u)], right_relay, right_beyond.at[u // parts], rows=partner)

    def kept(u):
        i, j = spot(u)
        slot = lax.rem(u, depth)
        return [
            pltpu.make_async_copy(done.at[slot, 1], rights.at[r, at(u)], done_sem.at[slot, 6]),
            pltpu.make_async_copy(ready.at[slot, 0], state1.at[i, j], done_sem.at[slot, 7]),
            pltpu.make_async_copy(ready.at[slot, 1], gate1.at[i, j], done_sem.at[slot, 8]),
        ]

    def each_send(u, act):
        @pl.when(c < last)
        def _():
            act(line_right(u, 0), True)

        @pl.when(c > 0)
        def _():
            act(line_left(u, 0), True)

        @pl.when(c != r)
        def _():
            act(own_spread(u), True)

        @pl.when(c == r)
        def _():
            act(own_keep(u), False)

        act(right_to_across(u), True)
        act(right_to_partner(u), True)
        for copy in kept(u):
            act(copy, False)

    start = lambda copy, away: copy.start()
    sent = lambda copy, away: copy.wait_send() if away else copy.wait()
    few = next(k for k in (8, 6, 4, 3, 2, 1) if mi % k == 0)

    def update(u):
        slot, out = lax.rem(u, 4), lax.rem(u, depth)
        p, q = u // parts, lax.rem(u, parts)
        count = few * m

        @pl.loop(0, mi // few)
        def _(g):
            rows_at = pl.ds(g * few, few)
            mixed = chunk[slot, c, rows_at].reshape(count, LANES)
            result = times(normalize(mixed, out_gain[0:1, :], out_bias[0:1, :]), out3[...])
            new = tile[0, rows_at].reshape(count, LANES) + tile[1, rows_at].reshape(count, LANES) * result
            normed = normalize(new, norm_gain[1:2, :], norm_bias[1:2, :])
            row_first = r * extent + q * mi + g * few
            col_part = tokens[pl.ds(pl.multiple_of(c * extent + p * m, 8), m), :]
            mask = jnp.concatenate(
                [tokens[pl.ds(row_first + b, 1), :] * col_part for b in range(few)], axis=0
            )
            left, right, gating = gated_three(normed, mask, proj3[...])
            for k, value in enumerate((left, right)):
                done[out, k, pl.ds(pl.multiple_of(g * count, 8), count), :] = value
            for k, value in enumerate((new, gating)):
                ready[out, k, rows_at] = value.reshape(few, m, LANES)

    def pass_line(u, s):
        @pl.when(c >= s)
        def _():
            line_right_in(u, s - 1).wait_recv()
            if s < last:
                @pl.when(c < last)
                def _():
                    line_right(u, s).start()
            spread(u, c - s)

        @pl.when(back >= s)
        def _():
            line_left_in(u, s - 1).wait_recv()
            if s < last:
                @pl.when(back < last)
                def _():
                    line_left(u, s).start()
            spread(u, c + s)

    def line_right_in(u, s):
        return remote(done.at[0, 0], line.at[c - 1 - s, at(u)], forward_sem.at[0], line_recv_r.at[u, s], cols=c - 1)

    def line_left_in(u, s):
        return remote(done.at[0, 0], line.at[c + 1 + s, at(u)], forward_sem.at[1], line_recv_l.at[u, s], cols=c + 1)

    def spread(u, origin):
        @pl.when(origin != r)
        def _():
            remote(
                line.at[origin, at(u)], lefts.at[r, at(u)], spread_sem, left_recv.at[r, u // parts], rows=origin
            ).start()

    wide = rows * extent // LANES
    share = extent * m

    def piece(p):
        return pl.ds(p * share, share)

    def fetch(which, p):
        span = piece(p)
        for o in range(rows):
            if which:
                pltpu.make_async_copy(rights.at[o, span], fetched(o), load_sem.at[o]).start()
            else:
                @pl.when(r == o)
                def _():
                    pltpu.make_async_copy(line.at[o, span], fetched(o), load_sem.at[o]).start()

                @pl.when(r != o)
                def _():
                    pltpu.make_async_copy(lefts.at[o, span], fetched(o), load_sem.at[o]).start()

    def fetched(o):
        return block.at[pl.ds(o * share, share)]

    def arrived(which, p):
        span = piece(p)

        def settle(ref, o, sem):
            pltpu.make_async_copy(ref.at[o, span], ref.at[o, span], sem).wait()

        if which:
            settle(rights, partner, right_near.at[p])
            settle(rights, beyond, right_beyond.at[p])
        else:
            for o in range(rows):
                @pl.when(r != o)
                def _():
                    settle(lefts, o, left_recv.at[o, p])

    def put(which, p):
        target = right_k if which else near
        return [pltpu.make_async_copy(stage.at[w], target.at[w, p], stage_sem.at[w]) for w in range(wide)]

    def along(which, p, before):
        for o in range(rows):
            pltpu.make_async_copy(rights.at[o, piece(p)], fetched(o), load_sem.at[o]).wait()
        if before is not None:
            for copy in put(*before):
                copy.wait()

        @pl.loop(0, m)
        def _(i):
            for w in range(wide):
                got = block[pl.ds(w * LANES * m + i, LANES, m), :].T
                stage[w, pl.ds(i, LANES, m), :] = got

        for copy in put(which, p):
            copy.start()

    def within(u):
        return jnp.logical_and(u >= 0, u < ticks)

    order = [(0, p) for p in range(n)] + [(1, p) for p in range(n)]
    late = 4
    known = lambda which, p: (p + 1) * parts - 1 + last + max(late + 2, depth)
    turns = ticks + last + max(depth, late, last + 1)
    order.sort(key=lambda step: known(*step))
    begins = []
    for step in order:
        begins.append(max(known(*step), begins[-1] + 1 if begins else ticks - parts))
    steps, ending = [], []
    for k, (which, p) in enumerate(order):
        before = order[k - 1] if k else None

        def begin(which=which, p=p):
            arrived(which, p)
            fetch(which, p)

        def close(which=which, p=p, before=before):
            along(which, p, before)

        for when, act in ((begins[k], begin), (begins[k] + 1, close)):
            if when < turns:
                steps.append((when, act))
            else:
                ending.append(act)
    steps.sort(key=lambda step: step[0])

    half_way = parts // 2
    some = LANES // (parts - half_way)
    for k in range(cuts):
        near_copy, far_copy, on_copy = early(k)
        far_copy.wait_recv()
        on_copy.start()
        near_copy.wait_recv()
        on_copy.wait_recv()
        for copy in early_loads(k):
            copy.start()
        for copy in early_loads(k):
            copy.wait()
        multiply(0, k * cut, cut)
    for k in range(cuts):
        for copy in early(k):
            copy.wait_send()

    @pl.loop(0, turns)
    def _(t):
        p, q = t // parts, lax.rem(t, parts)

        @pl.when(within(t - last))
        def _():
            for copy in tiles(t - last):
                copy.start()

        @pl.when(within(t - 4))
        def _():
            clear_sums(t - 4)

        @pl.when(t < ticks)
        def _():
            turn(p, q, lax.rem(t, 4))
            pass_sums(t, 0)

            @pl.when(p + 1 < n)
            def _():
                @pl.when(q == half_way - 2)
                def _():
                    to_across(p + 1).wait_recv()
                    relay(p + 1).start()

                @pl.when(q == half_way - 1)
                def _():
                    to_partner(p + 1).wait_recv()
                    relay(p + 1).wait_recv()
                    for copy in loads(p + 1):
                        copy.start()

                @pl.when(q == half_way)
                def _():
                    relay(p + 1).wait_send()
                    for copy in loads(p + 1):
                        copy.wait()

                @pl.when(q >= half_way)
                def _():
                    multiply(p + 1, (q - half_way) * some, some)

        for s in range(1, last):
            @pl.when(within(t - s))
            def _():
                pass_sums(t - s, s)

        for s in range(1, last + 1):
            @pl.when(within(t - last - s))
            def _():
                pass_line(t - last - s, s)

        u = t - last

        @pl.when(within(u - late))
        def _():
            right_to_across(u - late).wait_recv()
            right_on(u - late).start()

        @pl.when(within(u - depth))
        def _():
            each_send(u - depth, sent)

        for when, act in steps:
            @pl.when(t == when)
            def _():
                act()

        @pl.when(within(u))
        def _():
            own_sum(u)
            for copy in tiles(u):
                copy.wait()
            update(u)
            each_send(u, start)

    for act in ending:
        act()
    for copy in put(*order[-1]):
        copy.wait()
    for p in range(1, n):
        to_across(p).wait_send()
        to_partner(p).wait_send()

    def drain(sem, count):
        pltpu.make_async_copy(line.at[pl.ds(0, count)], line.at[pl.ds(0, count)], sem).wait()

    for count in range(1, last):
        @pl.when(c == count)
        def _():
            drain(forward_sem.at[0], count)

        @pl.when(back == count)
        def _():
            drain(forward_sem.at[1], count)

    drain(right_relay, 1)

    @pl.when(c == r)
    def _():
        drain(spread_sem, last)

    @pl.when(c != r)
    def _():
        drain(spread_sem, last - 1)


def middle_call(rows, cols, n, parts, state, *small):
    extent = state.shape[0]
    m, mi = extent // n, extent // parts
    ticks = n * parts
    last = cols - 1
    wide = rows * extent // LANES
    f32, bf16 = jnp.float32, jnp.bfloat16
    bit, flat = (mi, m, LANES), (mi * m, LANES)
    anywhere = pl.BlockSpec(memory_space=pl.ANY)
    inside = pl.BlockSpec(memory_space=pltpu.VMEM)
    dma = pltpu.SemaphoreType.DMA
    whole = jax.ShapeDtypeStruct((rows, extent * extent, LANES), f32)
    long = jax.ShapeDtypeStruct((wide, n, LANES * m, LANES), f32)
    square = jax.ShapeDtypeStruct(state.shape, f32)
    return pl.pallas_call(
        functools.partial(middle_kernel, rows, cols, n, parts),
        in_specs=[anywhere] + [inside] * len(small),
        out_specs=[anywhere] * 8,
        out_shape=[long, whole, whole, whole, long, square, square, square],
        scratch_shapes=[
            pltpu.VMEM((n, LANES * m, LANES), f32),
            pltpu.VMEM((2, m, extent, LANES), f32),
            pltpu.VMEM((2, m, extent, LANES), f32),
            pltpu.VMEM((3 * LANES, 5 * LANES), bf16),
            pltpu.VMEM((LANES, extent, LANES), bf16),
            pltpu.VMEM((LANES, extent, LANES), bf16),
            pltpu.VMEM((rows * max(LANES, extent) * m, LANES), f32),
            pltpu.VMEM((2, extent * LANES, LANES), f32),
            pltpu.VMEM((wide, LANES * m, LANES), f32),
            pltpu.VMEM((4, cols) + bit, f32),
            pltpu.VMEM((6, last) + bit, f32),
            pltpu.VMEM((6, last) + bit, f32),
            pltpu.VMEM((2,) + bit, f32),
            pltpu.VMEM((8, 2) + flat, f32),
            pltpu.VMEM((8, 2) + bit, f32),
            pltpu.VMEM((3 * LANES, LANES), bf16),
            pltpu.VMEM((3 * LANES, 5 * LANES), bf16),
            dma((2,)), dma((2,)), dma((3, 4)), dma((3, 4)), dma((3, n)), dma((3, n)), dma((max(n, rows),)), dma((2,)),
            dma((4, last)), dma((4, last)), dma((6, last)), dma((6, last)),
            dma((ticks, last)), dma((ticks, last)), dma((8, 9)), dma((2,)), dma,
            dma((rows, n)), dma((n,)), dma((ticks,)), dma((n,)), dma, dma((wide,)),
        ],
        compiler_params=pltpu.CompilerParams(
            collective_id=0, has_side_effects=True, vmem_limit_bytes=VMEM_LIMIT
        ),
    )(state, *small)


def last_kernel(left_k, right_k, state1, gate1, out_gain, out_bias, out_weight, out, turned, ends, out3, end_sem):
    g, steps = pl.program_id(0), pl.num_programs(0)
    wide, n, block, _ = left_k.shape
    size = ends.shape[1]
    extent = turned.shape[0] // LANES
    m = extent // n
    heads = block // m
    copies = [pltpu.make_async_copy(source, ends.at[k], end_sem.at[k]) for k, source in enumerate((state1, gate1))]

    @pl.when(g == 0)
    def _():
        for copy in copies:
            copy.start()
        stack_into(out3, 0, out_weight[1])

    def rows_of(ref, b, w):
        return jnp.concatenate([ref[w, p, b * m : (b + 1) * m, :] for p in range(n)], axis=0)

    for b in range(heads):
        a = [halves(rows_of(left_k, b, w)) for w in range(wide)]
        k = [halves(padded(rows_of(right_k, b, w))) for w in range(wide)]
        a3 = jnp.concatenate([x[0] for x in a] + [x[1] for x in a] + [x[0] for x in a], axis=1)
        k3 = jnp.concatenate([x[0] for x in k] + [x[0] for x in k] + [x[1] for x in k], axis=1)
        turned[pl.ds(g * heads + b, extent, LANES), :] = against(a3, k3)

    @pl.when(g == steps - 1)
    def _():
        for copy in copies:
            copy.wait()
        few = 4

        @pl.loop(0, extent // few)
        def _(i):
            straight = [
                turned[pl.ds(pl.multiple_of((i * few + b) * LANES, LANES), LANES), :].T[:extent]
                for b in range(few)
            ]
            mixed = jnp.concatenate(straight, axis=0)
            result = times(normalize(mixed, out_gain[1:2, :], out_bias[1:2, :]), out3[...])
            at = pl.ds(pl.multiple_of(i * few * extent, 8), few * extent)
            out[at, :] = ends[0, at, :] + ends[1, at, :] * result


def last_call(left_k, right_k, state1, gate1, *small):
    extent = state1.shape[0]
    wide, n, _, _ = left_k.shape
    size = extent * extent
    f32 = jnp.float32
    heads = 8
    part = pl.BlockSpec((wide, n, heads * (extent // n), LANES), lambda g: (0, 0, g, 0))
    anywhere = pl.BlockSpec(memory_space=pl.ANY)
    out = pl.pallas_call(
        last_kernel,
        grid=(LANES // heads,),
        in_specs=[part, part, anywhere, anywhere]
        + [pl.BlockSpec(a.shape, lambda g, a=a: (0,) * a.ndim) for a in small],
        out_specs=pl.BlockSpec((size, LANES), lambda g: (0, 0)),
        out_shape=jax.ShapeDtypeStruct((size, LANES), f32),
        scratch_shapes=[
            pltpu.VMEM((extent * LANES, LANES), f32),
            pltpu.VMEM((2, size, LANES), f32),
            pltpu.VMEM((3 * LANES, LANES), jnp.bfloat16),
            pltpu.SemaphoreType.DMA((2,)),
        ],
        compiler_params=pltpu.CompilerParams(vmem_limit_bytes=VMEM_LIMIT),
    )(left_k, right_k, state1.reshape(size, LANES), gate1.reshape(size, LANES), *small)
    return out.reshape(extent, extent, LANES)


def body(rows, cols, pieces, parts, pair_state, token_mask, norm_gain, norm_bias, proj_weight,
         gate_weight, out_gain, out_bias, out_weight):
    tokens = jnp.broadcast_to(token_mask.astype(jnp.float32)[:, None], (token_mask.shape[0], LANES))
    left_k, _, _, _, right_k, state1, gate1, _ = middle_call(
        rows, cols, pieces, parts, pair_state, tokens,
        norm_gain, norm_bias, proj_weight, gate_weight, out_gain, out_bias, out_weight,
    )
    return last_call(left_k, right_k, state1, gate1, out_gain, out_bias, out_weight)


def solution(mesh):
    placed = (P(("groups", "rows"), "cols", None), P("groups"), P(), P(), P(), P(), P(), P(), P())
    rows, cols = mesh.shape["rows"], mesh.shape["cols"]

    def run(pair_state, *rest):
        proj_weight = rest[3]
        channels, hidden = pair_state.shape[2], proj_weight.shape[2] // 4
        extent = pair_state.shape[0]
        fits = channels == hidden == LANES and extent == pair_state.shape[1] and extent <= LANES
        if rows == cols == 4 and fits and extent % (8 * rows) == 0:
            return body(rows, cols, rows, 2 * rows, pair_state, *rest)
        return plain_body(pair_state, *rest)

    return jax.shard_map(
        run,
        mesh=mesh,
        in_specs=placed,
        out_specs=P(("groups", "rows"), "cols", None),
        check_vma=False,
    )
```

```python
import functools

import jax
import jax.numpy as jnp
from jax import lax
from jax.experimental import pallas as pl
from jax.experimental.pallas import tpu as pltpu
from jax.sharding import PartitionSpec as P

eps = 1e-05
precise = lax.Precision.HIGH
MESH = pl.DeviceIdType.MESH
LANES = 128
VMEM_LIMIT = 67_000_000


def normalize(values, gain, shift):
    center = values - jnp.mean(values, axis=-1, keepdims=True)
    spread = jnp.mean(center * center, axis=-1, keepdims=True)
    return center * lax.rsqrt(spread + eps) * gain + shift


def project(state, pair_mask, segment, norm_gain, norm_bias, proj_weight, gate_weight):
    width = proj_weight.shape[2] // 4
    normed = normalize(state, norm_gain[segment], norm_bias[segment])
    hidden = jnp.einsum(
        "ijc,cf->ijf", normed, proj_weight[segment], precision=precise
    )
    left_side = (
        pair_mask[:, :, None]
        * jax.nn.sigmoid(hidden[:, :, :width])
        * hidden[:, :, width : 2 * width]
    )
    right_side = (
        pair_mask[:, :, None]
        * jax.nn.sigmoid(hidden[:, :, 2 * width : 3 * width])
        * hidden[:, :, 3 * width :]
    )
    gating = jax.nn.sigmoid(
        jnp.einsum("ijc,cd->ijd", normed, gate_weight[segment], precision=precise)
    )
    return (left_side, right_side, gating)


def finish(state, mixed, gating, segment, out_gain, out_bias, out_weight):
    result = jnp.einsum(
        "ijh,hc->ijc",
        normalize(mixed, out_gain[segment], out_bias[segment]),
        out_weight[segment],
        precision=precise,
    )
    return state + gating * result


def plain_body(
    pair_state,
    token_mask,
    norm_gain,
    norm_bias,
    proj_weight,
    gate_weight,
    out_gain,
    out_bias,
    out_weight,
):
    row_count = pair_state.shape[0]
    col_count = pair_state.shape[1]
    row_start = lax.axis_index("rows") * row_count
    col_start = lax.axis_index("cols") * col_count
    maskf = token_mask.astype(jnp.float32)
    row_mask = lax.dynamic_slice_in_dim(maskf, row_start, row_count)
    col_mask = lax.dynamic_slice_in_dim(maskf, col_start, col_count)
    pair_mask = row_mask[:, None] * col_mask[None, :]
    left_side, right_side, gating = project(
        pair_state, pair_mask, 0, norm_gain, norm_bias, proj_weight, gate_weight
    )
    partial_out = jnp.einsum(
        "ikh,jkh->ijh",
        left_side,
        lax.all_gather(right_side, "rows", axis=0, tiled=True),
        precision=precise,
    )
    mixed = lax.psum_scatter(partial_out, "cols", scatter_dimension=1, tiled=True)
    updated = finish(pair_state, mixed, gating, 0, out_gain, out_bias, out_weight)
    left_next, right_next, gate_next = project(
        updated, pair_mask, 1, norm_gain, norm_bias, proj_weight, gate_weight
    )
    partial_in = jnp.einsum(
        "kih,kjh->ijh",
        lax.all_gather(left_next, "cols", axis=1, tiled=True),
        right_next,
        precision=precise,
    )
    mixed_next = lax.psum_scatter(partial_in, "rows", scatter_dimension=0, tiled=True)
    return finish(updated, mixed_next, gate_next, 1, out_gain, out_bias, out_weight)


def halves(x):
    high = x.astype(jnp.bfloat16)
    return high, (x - high.astype(jnp.float32)).astype(jnp.bfloat16)


def streamed(x):
    high, low = halves(x)
    return jnp.concatenate([high, low, high], axis=1)


def held(x):
    high, low = halves(x)
    return jnp.concatenate([high, high, low], axis=1)


def stack_into(target, first, weight):
    high, low = halves(weight)
    for k, part in enumerate((high, high, low)):
        target[k * LANES : (k + 1) * LANES, first : first + weight.shape[1]] = part


def times(x, weight3):
    return jnp.dot(streamed(x), weight3, preferred_element_type=jnp.float32)


def against(a3, b3):
    return lax.dot_general(
        a3, b3, (((1,), (1,)), ((), ())), preferred_element_type=jnp.float32
    )


def gated_three(normed, mask, weight3):
    hidden = times(normed, weight3)
    part = lambda f: hidden[:, f * LANES : (f + 1) * LANES]
    return (
        mask * jax.nn.sigmoid(part(0)) * part(1),
        mask * jax.nn.sigmoid(part(2)) * part(3),
        jax.nn.sigmoid(part(4)),
    )


def across_lanes(x):
    short = LANES - x.shape[1]
    if short == 0:
        return x
    return jnp.concatenate([x, jnp.zeros((x.shape[0], short), x.dtype)], axis=1)


def padded(x):
    rows = x.shape[0]
    if rows == LANES:
        return x
    return jnp.concatenate([x, jnp.zeros((LANES - rows, x.shape[1]), x.dtype)], axis=0)


def middle_kernel(
    rows, cols, n, parts,
    state, tokens, norm_gain, norm_bias, proj, gate_weight, out_gain, out_bias, out_weight,
    near, line, lefts, rights, right_k, state1, gate1, gate0,
    mine, first, opened, first3, high, low, block, turned, stage, chunk, from_left, from_right, tile, done, ready, out3, proj3,
    first_sem, opened_sem, early_send, early_recv, gather_send, gather_recv, load_sem, tile_sem,
    sum_send_r, sum_send_l, sum_recv_r, sum_recv_l,
    line_recv_r, line_recv_l, done_sem, forward_sem, spread_sem, left_recv,
    right_near, right_across, right_beyond, right_relay, stage_sem,
):
    mi, m = tile.shape[1:3]
    extent = n * m
    ticks = n * parts
    last = cols - 1
    r, c = lax.axis_index("rows"), lax.axis_index("cols")
    back = last - c
    depth, ring = done.shape[0], from_left.shape[0]
    partner = r + 1 - 2 * lax.rem(r, 2)
    across = lax.rem(r + 2, rows)
    beyond = lax.rem(partner + 2, rows)

    def opening(p):
        return pltpu.make_async_copy(state.at[pl.ds(p * m, m)], first.at[p % 2], first_sem.at[p % 2])

    opening(0).start()
    stack_into(first3, 0, proj[0])
    stack_into(first3, 4 * LANES, gate_weight[0])
    stack_into(out3, 0, out_weight[0])
    stack_into(proj3, 0, proj[1])
    stack_into(proj3, 4 * LANES, gate_weight[1])

    barrier = pltpu.get_barrier_semaphore()
    for off in range(1, rows):
        pl.semaphore_signal(barrier, inc=1, device_id={"rows": lax.rem(r + off, rows)}, device_id_type=MESH)

    @pl.when(c > 0)
    def _():
        pl.semaphore_signal(barrier, inc=1, device_id={"cols": c - 1}, device_id_type=MESH)

    @pl.when(c < last)
    def _():
        pl.semaphore_signal(barrier, inc=1, device_id={"cols": c + 1}, device_id_type=MESH)

    pl.semaphore_wait(barrier, rows - 1 + jnp.minimum(c, 1) + jnp.minimum(back, 1))

    def remote(src, dst, send, recv, **where):
        return pltpu.make_async_remote_copy(
            src_ref=src, dst_ref=dst, send_sem=send, recv_sem=recv,
            device_id=where, device_id_type=MESH,
        )

    def to_partner(p):
        return remote(mine.at[p], near.at[0, p], gather_send.at[0, p], gather_recv.at[0, p], rows=partner)

    def to_across(p):
        return remote(mine.at[p], near.at[1, p], gather_send.at[1, p], gather_recv.at[1, p], rows=across)

    def relay(p):
        return remote(near.at[1, p], near.at[2, p], gather_send.at[2, p], gather_recv.at[2, p], rows=partner)

    def slab(o):
        return block.at[pl.ds(pl.multiple_of(o * LANES * m, 8), LANES * m)]

    def loads(p):
        return [
            pltpu.make_async_copy(mine.at[p], slab(r), load_sem.at[0]),
            pltpu.make_async_copy(near.at[0, p], slab(partner), load_sem.at[1]),
            pltpu.make_async_copy(near.at[1, p], slab(across), load_sem.at[2]),
            pltpu.make_async_copy(near.at[2, p], slab(beyond), load_sem.at[3]),
        ]

    cuts = 4
    cut = LANES // cuts

    def part(k):
        return pl.ds(k * cut * m, cut * m)

    def early(k):
        return (
            remote(mine.at[0, part(k)], near.at[0, 0, part(k)], early_send.at[0, k], early_recv.at[0, k], rows=partner),
            remote(mine.at[0, part(k)], near.at[1, 0, part(k)], early_send.at[1, k], early_recv.at[1, k], rows=across),
            remote(near.at[1, 0, part(k)], near.at[2, 0, part(k)], early_send.at[2, k], early_recv.at[2, k], rows=partner),
        )

    def early_loads(k):
        return [
            pltpu.make_async_copy(
                source.at[0, part(k)],
                block.at[pl.ds(pl.multiple_of(o * LANES * m + k * cut * m, 8), cut * m)],
                load_sem.at[b],
            )
            for b, (source, o) in enumerate(
                ((mine, r), (near.at[0], partner), (near.at[1], across), (near.at[2], beyond))
            )
        ]

    def closing(p):
        return pltpu.make_async_copy(opened.at[p % 2], gate0.at[pl.ds(p * m, m)], opened_sem.at[p % 2])

    group = 4
    taken = group * extent
    for p in range(n):
        opening(p).wait()
        if p + 1 < n:
            opening(p + 1).start()
        if p >= 2:
            closing(p - 2).wait()

        @pl.loop(0, m // group)
        def _(g):
            rows_at = pl.ds(g * group, group)
            normed = normalize(first[p % 2, rows_at].reshape(taken, LANES), norm_gain[0:1, :], norm_bias[0:1, :])
            row_first = r * extent + p * m + g * group
            col_part = tokens[pl.ds(pl.multiple_of(c * extent, 8), extent), :]
            mask = jnp.concatenate(
                [tokens[pl.ds(row_first + b, 1), :] * col_part for b in range(group)], axis=0
            )
            left, right, gating = gated_three(normed, mask, first3[...])
            opened[p % 2, rows_at] = gating.reshape(group, extent, LANES)
            for b in range(group):
                span = slice(b * extent, (b + 1) * extent)
                mine[p, pl.ds(g * group + b, LANES, m), :] = padded(right[span]).T
                turned[1, pl.ds(p * LANES * m + g * group + b, LANES, m), :] = padded(left[span]).T

        closing(p).start()
        if p:
            if p <= 1:
                to_across(p).start()
                to_partner(p).start()
        else:
            for k in range(cuts):
                for copy in early(k)[1::-1]:
                    copy.start()
    for p in range(max(n - 2, 0), n):
        closing(p).wait()

    @pl.loop(0, LANES)
    def _(h):
        rows_of = [
            turned[1, pl.ds(pl.multiple_of(p * LANES * m + h * m, 8), m), :] for p in range(n)
        ]
        top, rest = halves(jnp.concatenate(rows_of, axis=0))
        high[h] = top
        low[h] = rest

    def multiply(p, start_at, count):
        half = lax.rem(p, 2)

        @pl.loop(start_at // 4, (start_at + count) // 4)
        def _(g):
            for b in range(4):
                h = g * 4 + b
                right = jnp.concatenate(
                    [block[pl.ds(pl.multiple_of(o * LANES * m + h * m, 8), m), :] for o in range(rows)], axis=0
                )
                a3 = jnp.concatenate([high[h], low[h], high[h]], axis=1)
                turned[half, pl.ds(h, extent, LANES), :] = across_lanes(against(a3, held(right)))

    def turn(p, q, slot):
        @pl.loop(0, mi)
        def _(i):
            at = pl.multiple_of((q * mi + i) * LANES, LANES)
            straight = turned[lax.rem(p, 2), pl.ds(at, LANES), :].T
            for d in range(cols):
                chunk[slot, d, i] = straight[d * m : (d + 1) * m]

    def sum_right(u, s):
        slot = lax.rem(u, 4)
        return remote(chunk.at[slot, c + last - s], from_left.at[lax.rem(u, ring), s], sum_send_r.at[slot, s], sum_recv_r.at[lax.rem(u, ring), s], cols=c + 1)

    def sum_left(u, s):
        slot = lax.rem(u, 4)
        return remote(chunk.at[slot, c - last + s], from_right.at[lax.rem(u, ring), s], sum_send_l.at[slot, s], sum_recv_l.at[lax.rem(u, ring), s], cols=c - 1)

    def arrived_right(u, s):
        return remote(chunk.at[0, 0], from_left.at[lax.rem(u, ring), s], sum_send_r.at[0, s], sum_recv_r.at[lax.rem(u, ring), s], cols=c - 1)

    def arrived_left(u, s):
        return remote(chunk.at[0, 0], from_right.at[lax.rem(u, ring), s], sum_send_l.at[0, s], sum_recv_l.at[lax.rem(u, ring), s], cols=c + 1)

    def add_to(slot, d, source, u, s):
        @pl.loop(0, mi)
        def _(i):
            chunk[slot, d, i] = chunk[slot, d, i] + source[lax.rem(u, ring), s, i]

    def pass_sums(u, s):
        slot = lax.rem(u, 4)

        @pl.when(c <= s)
        def _():
            if s:
                @pl.when(c > 0)
                def _():
                    arrived_right(u, s - 1).wait_recv()
                    add_to(slot, c + last - s, from_left, u, s - 1)
            sum_right(u, s).start()

        @pl.when(back <= s)
        def _():
            if s:
                @pl.when(back > 0)
                def _():
                    arrived_left(u, s - 1).wait_recv()
                    add_to(slot, c - last + s, from_right, u, s - 1)
            sum_left(u, s).start()

    def clear_sums(u):
        for s in range(last):
            @pl.when(c <= s)
            def _():
                sum_right(u, s).wait_send()

            @pl.when(back <= s)
            def _():
                sum_left(u, s).wait_send()

    def own_sum(u):
        slot = lax.rem(u, 4)

        @pl.when(c > 0)
        def _():
            arrived_right(u, last - 1).wait_recv()
            add_to(slot, c, from_left, u, last - 1)

        @pl.when(c < last)
        def _():
            arrived_left(u, last - 1).wait_recv()
            add_to(slot, c, from_right, u, last - 1)

    def spot(u):
        p, q = u // parts, lax.rem(u, parts)
        return pl.ds(q * mi, mi), pl.ds(pl.multiple_of(p * m, 8), m)

    def tiles(u):
        i, j = spot(u)
        return [
            pltpu.make_async_copy(state.at[i, j], tile.at[0], tile_sem.at[0]),
            pltpu.make_async_copy(gate0.at[i, j], tile.at[1], tile_sem.at[1]),
        ]

    def at(u):
        return pl.ds(pl.multiple_of(u * mi * m, 8), mi * m)

    def line_right(u, s):
        src = done.at[lax.rem(u, depth), 0] if s == 0 else line.at[c - s, at(u)]
        send = done_sem.at[lax.rem(u, depth), 0] if s == 0 else forward_sem.at[0]
        return remote(src, line.at[c - s, at(u)], send, line_recv_r.at[u, s], cols=c + 1)

    def line_left(u, s):
        src = done.at[lax.rem(u, depth), 0] if s == 0 else line.at[c + s, at(u)]
        send = done_sem.at[lax.rem(u, depth), 1] if s == 0 else forward_sem.at[1]
        return remote(src, line.at[c + s, at(u)], send, line_recv_l.at[u, s], cols=c - 1)

    def own_spread(u):
        return remote(done.at[lax.rem(u, depth), 0], lefts.at[r, at(u)], done_sem.at[lax.rem(u, depth), 2], left_recv.at[r, u // parts], rows=c)

    def own_keep(u):
        return pltpu.make_async_copy(done.at[lax.rem(u, depth), 0], line.at[c, at(u)], done_sem.at[lax.rem(u, depth), 3])

    def right_to_partner(u):
        return remote(done.at[lax.rem(u, depth), 1], rights.at[r, at(u)], done_sem.at[lax.rem(u, depth), 4], right_near.at[u // parts], rows=partner)

    def right_to_across(u):
        return remote(done.at[lax.rem(u, depth), 1], rights.at[r, at(u)], done_sem.at[lax.rem(u, depth), 5], right_across.at[u], rows=across)

    def right_on(u):
        return remote(rights.at[across, at(u)], rights.at[across, at(u)], right_relay, right_beyond.at[u // parts], rows=partner)

    def kept(u):
        i, j = spot(u)
        slot = lax.rem(u, depth)
        return [
            pltpu.make_async_copy(done.at[slot, 1], rights.at[r, at(u)], done_sem.at[slot, 6]),
            pltpu.make_async_copy(ready.at[slot, 0], state1.at[i, j], done_sem.at[slot, 7]),
            pltpu.make_async_copy(ready.at[slot, 1], gate1.at[i, j], done_sem.at[slot, 8]),
        ]

    def each_send(u, act):
        @pl.when(c < last)
        def _():
            act(line_right(u, 0), True)

        @pl.when(c > 0)
        def _():
            act(line_left(u, 0), True)

        @pl.when(c != r)
        def _():
            act(own_spread(u), True)

        @pl.when(c == r)
        def _():
            act(own_keep(u), False)

        act(right_to_across(u), True)
        act(right_to_partner(u), True)
        for copy in kept(u):
            act(copy, False)

    start = lambda copy, away: copy.start()
    sent = lambda copy, away: copy.wait_send() if away else copy.wait()
    few = next(k for k in (8, 6, 4, 3, 2, 1) if mi % k == 0)

    def update(u):
        slot, out = lax.rem(u, 4), lax.rem(u, depth)
        p, q = u // parts, lax.rem(u, parts)
        count = few * m

        @pl.loop(0, mi // few)
        def _(g):
            rows_at = pl.ds(g * few, few)
            mixed = chunk[slot, c, rows_at].reshape(count, LANES)
            result = times(normalize(mixed, out_gain[0:1, :], out_bias[0:1, :]), out3[...])
            new = tile[0, rows_at].reshape(count, LANES) + tile[1, rows_at].reshape(count, LANES) * result
            normed = normalize(new, norm_gain[1:2, :], norm_bias[1:2, :])
            row_first = r * extent + q * mi + g * few
            col_part = tokens[pl.ds(pl.multiple_of(c * extent + p * m, 8), m), :]
            mask = jnp.concatenate(
                [tokens[pl.ds(row_first + b, 1), :] * col_part for b in range(few)], axis=0
            )
            left, right, gating = gated_three(normed, mask, proj3[...])
            for k, value in enumerate((left, right)):
                done[out, k, pl.ds(pl.multiple_of(g * count, 8), count), :] = value
            for k, value in enumerate((new, gating)):
                ready[out, k, rows_at] = value.reshape(few, m, LANES)

    def pass_line(u, s):
        @pl.when(c >= s)
        def _():
            line_right_in(u, s - 1).wait_recv()
            if s < last:
                @pl.when(c < last)
                def _():
                    line_right(u, s).start()
            spread(u, c - s)

        @pl.when(back >= s)
        def _():
            line_left_in(u, s - 1).wait_recv()
            if s < last:
                @pl.when(back < last)
                def _():
                    line_left(u, s).start()
            spread(u, c + s)

    def line_right_in(u, s):
        return remote(done.at[0, 0], line.at[c - 1 - s, at(u)], forward_sem.at[0], line_recv_r.at[u, s], cols=c - 1)

    def line_left_in(u, s):
        return remote(done.at[0, 0], line.at[c + 1 + s, at(u)], forward_sem.at[1], line_recv_l.at[u, s], cols=c + 1)

    def spread(u, origin):
        @pl.when(origin != r)
        def _():
            remote(
                line.at[origin, at(u)], lefts.at[r, at(u)], spread_sem, left_recv.at[r, u // parts], rows=origin
            ).start()

    wide = rows * extent // LANES
    share = extent * m

    def piece(p):
        return pl.ds(p * share, share)

    def fetch(which, p):
        span = piece(p)
        for o in range(rows):
            if which:
                pltpu.make_async_copy(rights.at[o, span], fetched(o), load_sem.at[o]).start()
            else:
                @pl.when(r == o)
                def _():
                    pltpu.make_async_copy(line.at[o, span], fetched(o), load_sem.at[o]).start()

                @pl.when(r != o)
                def _():
                    pltpu.make_async_copy(lefts.at[o, span], fetched(o), load_sem.at[o]).start()

    def fetched(o):
        return block.at[pl.ds(o * share, share)]

    def arrived(which, p):
        span = piece(p)

        def settle(ref, o, sem):
            pltpu.make_async_copy(ref.at[o, span], ref.at[o, span], sem).wait()

        if which:
            settle(rights, partner, right_near.at[p])
            settle(rights, beyond, right_beyond.at[p])
        else:
            for o in range(rows):
                @pl.when(r != o)
                def _():
                    settle(lefts, o, left_recv.at[o, p])

    def put(which, p):
        target = right_k if which else near
        return [pltpu.make_async_copy(stage.at[w], target.at[w, p], stage_sem.at[w]) for w in range(wide)]

    def along(which, p, before):
        for o in range(rows):
            pltpu.make_async_copy(rights.at[o, piece(p)], fetched(o), load_sem.at[o]).wait()
        if before is not None:
            for copy in put(*before):
                copy.wait()

        @pl.loop(0, m)
        def _(i):
            for w in range(wide):
                got = block[pl.ds(w * LANES * m + i, LANES, m), :].T
                stage[w, pl.ds(i, LANES, m), :] = got

        for copy in put(which, p):
            copy.start()

    def within(u):
        return jnp.logical_and(u >= 0, u < ticks)

    order = [(0, p) for p in range(n)] + [(1, p) for p in range(n)]
    late = 6
    known = lambda which, p: (p + 1) * parts - 1 + last + max(late + 2, depth)
    turns = ticks + last + max(depth, late, last + 1)
    order.sort(key=lambda step: known(*step))
    begins = []
    for step in order:
        begins.append(max(known(*step), begins[-1] + 1 if begins else ticks - parts))
    steps, ending = [], []
    for k, (which, p) in enumerate(order):
        before = order[k - 1] if k else None

        def begin(which=which, p=p):
            arrived(which, p)
            fetch(which, p)

        def close(which=which, p=p, before=before):
            along(which, p, before)

        for when, act in ((begins[k], begin), (begins[k] + 1, close)):
            if when < turns:
                steps.append((when, act))
            else:
                ending.append(act)
    steps.sort(key=lambda step: step[0])

    share_of = 1 << ((parts // 2).bit_length() - 1)
    half_way = parts - share_of
    some = LANES // share_of
    for k in range(cuts):
        near_copy, far_copy, on_copy = early(k)
        far_copy.wait_recv()
        on_copy.start()
        near_copy.wait_recv()
        on_copy.wait_recv()
        for copy in early_loads(k):
            copy.start()
        for copy in early_loads(k):
            copy.wait()
        multiply(0, k * cut, cut)
    for k in range(cuts):
        for copy in early(k):
            copy.wait_send()

    @pl.loop(0, turns)
    def _(t):
        p, q = t // parts, lax.rem(t, parts)

        @pl.when(within(t - last))
        def _():
            for copy in tiles(t - last):
                copy.start()

        @pl.when(within(t - 4))
        def _():
            clear_sums(t - 4)

        @pl.when(t < ticks)
        def _():
            turn(p, q, lax.rem(t, 4))
            pass_sums(t, 0)

            @pl.when(jnp.logical_and(q == 0, p + 2 < n))
            def _():
                to_across(p + 2).start()
                to_partner(p + 2).start()

            @pl.when(p + 1 < n)
            def _():
                @pl.when(q == half_way - 2)
                def _():
                    to_across(p + 1).wait_recv()
                    relay(p + 1).start()

                @pl.when(q == half_way - 1)
                def _():
                    to_partner(p + 1).wait_recv()
                    relay(p + 1).wait_recv()
                    for copy in loads(p + 1):
                        copy.start()

                @pl.when(q == half_way)
                def _():
                    relay(p + 1).wait_send()
                    for copy in loads(p + 1):
                        copy.wait()

                @pl.when(q >= half_way)
                def _():
                    multiply(p + 1, (q - half_way) * some, some)

        for s in range(1, last):
            @pl.when(within(t - s))
            def _():
                pass_sums(t - s, s)

        for s in range(1, last + 1):
            @pl.when(within(t - last - s))
            def _():
                pass_line(t - last - s, s)

        u = t - last

        @pl.when(within(u - late))
        def _():
            right_to_across(u - late).wait_recv()
            right_on(u - late).start()

        @pl.when(within(u - depth))
        def _():
            each_send(u - depth, sent)

        for when, act in steps:
            @pl.when(t == when)
            def _():
                act()

        @pl.when(within(u))
        def _():
            own_sum(u)
            for copy in tiles(u):
                copy.wait()
            update(u)
            each_send(u, start)

    for act in ending:
        act()
    for copy in put(*order[-1]):
        copy.wait()
    for p in range(1, n):
        to_across(p).wait_send()
        to_partner(p).wait_send()

    def drain(sem, count):
        pltpu.make_async_copy(line.at[pl.ds(0, count)], line.at[pl.ds(0, count)], sem).wait()

    for count in range(1, last):
        @pl.when(c == count)
        def _():
            drain(forward_sem.at[0], count)

        @pl.when(back == count)
        def _():
            drain(forward_sem.at[1], count)

    drain(right_relay, 1)

    @pl.when(c == r)
    def _():
        drain(spread_sem, last)

    @pl.when(c != r)
    def _():
        drain(spread_sem, last - 1)


def middle_call(rows, cols, n, parts, state, *small):
    extent = state.shape[0]
    m, mi = extent // n, extent // parts
    ticks = n * parts
    last = cols - 1
    wide = rows * extent // LANES
    f32, bf16 = jnp.float32, jnp.bfloat16
    bit, flat = (mi, m, LANES), (mi * m, LANES)
    anywhere = pl.BlockSpec(memory_space=pl.ANY)
    inside = pl.BlockSpec(memory_space=pltpu.VMEM)
    dma = pltpu.SemaphoreType.DMA
    whole = jax.ShapeDtypeStruct((rows, extent * extent, LANES), f32)
    long = jax.ShapeDtypeStruct((wide, n, LANES * m, LANES), f32)
    square = jax.ShapeDtypeStruct(state.shape, f32)
    return pl.pallas_call(
        functools.partial(middle_kernel, rows, cols, n, parts),
        in_specs=[anywhere] + [inside] * len(small),
        out_specs=[anywhere] * 8,
        out_shape=[long, whole, whole, whole, long, square, square, square],
        scratch_shapes=[
            pltpu.VMEM((n, LANES * m, LANES), f32),
            pltpu.VMEM((2, m, extent, LANES), f32),
            pltpu.VMEM((2, m, extent, LANES), f32),
            pltpu.VMEM((3 * LANES, 5 * LANES), bf16),
            pltpu.VMEM((LANES, extent, LANES), bf16),
            pltpu.VMEM((LANES, extent, LANES), bf16),
            pltpu.VMEM((rows * max(LANES, extent) * m, LANES), f32),
            pltpu.VMEM((2, extent * LANES, LANES), f32),
            pltpu.VMEM((wide, LANES * m, LANES), f32),
            pltpu.VMEM((4, cols) + bit, f32),
            pltpu.VMEM((6, last) + bit, f32),
            pltpu.VMEM((6, last) + bit, f32),
            pltpu.VMEM((2,) + bit, f32),
            pltpu.VMEM((8, 2) + flat, f32),
            pltpu.VMEM((8, 2) + bit, f32),
            pltpu.VMEM((3 * LANES, LANES), bf16),
            pltpu.VMEM((3 * LANES, 5 * LANES), bf16),
            dma((2,)), dma((2,)), dma((3, 4)), dma((3, 4)), dma((3, n)), dma((3, n)), dma((max(n, rows),)), dma((2,)),
            dma((4, last)), dma((4, last)), dma((6, last)), dma((6, last)),
            dma((ticks, last)), dma((ticks, last)), dma((8, 9)), dma((2,)), dma,
            dma((rows, n)), dma((n,)), dma((ticks,)), dma((n,)), dma, dma((wide,)),
        ],
        compiler_params=pltpu.CompilerParams(
            collective_id=0, has_side_effects=True, vmem_limit_bytes=VMEM_LIMIT
        ),
    )(state, *small)


def last_kernel(left_k, right_k, state1, gate1, out_gain, out_bias, out_weight, out, turned, ends, out3, end_sem):
    g, steps = pl.program_id(0), pl.num_programs(0)
    wide, n, block, _ = left_k.shape
    size = ends.shape[1]
    extent = turned.shape[0] // LANES
    m = extent // n
    heads = block // m
    copies = [pltpu.make_async_copy(source, ends.at[k], end_sem.at[k]) for k, source in enumerate((state1, gate1))]

    @pl.when(g == 0)
    def _():
        for copy in copies:
            copy.start()
        stack_into(out3, 0, out_weight[1])

    def rows_of(ref, b, w):
        return jnp.concatenate([ref[w, p, b * m : (b + 1) * m, :] for p in range(n)], axis=0)

    for b in range(heads):
        a = [halves(rows_of(left_k, b, w)) for w in range(wide)]
        k = [halves(rows_of(right_k, b, w)) for w in range(wide)]
        a3 = jnp.concatenate([x[0] for x in a] + [x[1] for x in a] + [x[0] for x in a], axis=1)
        k3 = jnp.concatenate([x[0] for x in k] + [x[0] for x in k] + [x[1] for x in k], axis=1)
        turned[pl.ds(g * heads + b, extent, LANES), :] = across_lanes(against(a3, k3))

    @pl.when(g == steps - 1)
    def _():
        for copy in copies:
            copy.wait()
        few = 4

        @pl.loop(0, extent // few)
        def _(i):
            straight = [
                turned[pl.ds(pl.multiple_of((i * few + b) * LANES, LANES), LANES), :].T[:extent]
                for b in range(few)
            ]
            mixed = jnp.concatenate(straight, axis=0)
            result = times(normalize(mixed, out_gain[1:2, :], out_bias[1:2, :]), out3[...])
            at = pl.ds(pl.multiple_of(i * few * extent, 8), few * extent)
            out[at, :] = ends[0, at, :] + ends[1, at, :] * result


def last_call(left_k, right_k, state1, gate1, *small):
    extent = state1.shape[0]
    wide, n, _, _ = left_k.shape
    size = extent * extent
    f32 = jnp.float32
    heads = 16
    part = pl.BlockSpec((wide, n, heads * (extent // n), LANES), lambda g: (0, 0, g, 0))
    anywhere = pl.BlockSpec(memory_space=pl.ANY)
    out = pl.pallas_call(
        last_kernel,
        grid=(LANES // heads,),
        in_specs=[part, part, anywhere, anywhere]
        + [pl.BlockSpec(a.shape, lambda g, a=a: (0,) * a.ndim) for a in small],
        out_specs=pl.BlockSpec((size, LANES), lambda g: (0, 0)),
        out_shape=jax.ShapeDtypeStruct((size, LANES), f32),
        scratch_shapes=[
            pltpu.VMEM((extent * LANES, LANES), f32),
            pltpu.VMEM((2, size, LANES), f32),
            pltpu.VMEM((3 * LANES, LANES), jnp.bfloat16),
            pltpu.SemaphoreType.DMA((2,)),
        ],
        compiler_params=pltpu.CompilerParams(vmem_limit_bytes=VMEM_LIMIT),
    )(left_k, right_k, state1.reshape(size, LANES), gate1.reshape(size, LANES), *small)
    return out.reshape(extent, extent, LANES)


def body(rows, cols, pieces, parts, pair_state, token_mask, norm_gain, norm_bias, proj_weight,
         gate_weight, out_gain, out_bias, out_weight):
    tokens = jnp.broadcast_to(token_mask.astype(jnp.float32)[:, None], (token_mask.shape[0], LANES))
    left_k, _, _, _, right_k, state1, gate1, _ = middle_call(
        rows, cols, pieces, parts, pair_state, tokens,
        norm_gain, norm_bias, proj_weight, gate_weight, out_gain, out_bias, out_weight,
    )
    return last_call(left_k, right_k, state1, gate1, out_gain, out_bias, out_weight)


def solution(mesh):
    placed = (P(("groups", "rows"), "cols", None), P("groups"), P(), P(), P(), P(), P(), P(), P())
    rows, cols = mesh.shape["rows"], mesh.shape["cols"]

    def run(pair_state, *rest):
        proj_weight = rest[3]
        channels, hidden = pair_state.shape[2], proj_weight.shape[2] // 4
        extent = pair_state.shape[0]
        fits = channels == hidden == LANES and extent == pair_state.shape[1] and extent <= LANES
        if rows == cols == 4 and fits and extent % (8 * rows) == 0:
            return body(rows, cols, 6, 8, pair_state, *rest)
        return plain_body(pair_state, *rest)

    return jax.shard_map(
        run,
        mesh=mesh,
        in_specs=placed,
        out_specs=P(("groups", "rows"), "cols", None),
        check_vma=False,
    )
```
